256 devices in a mesh: win: 2 (over z), trow: 128 (over y, x, core).
Axes of the slice: x: 8, y: 8, z: 2, core: 2. Of those that a mesh axis runs over, the one named last changes fastest.
The devices are a block of a 8x8x16 slice.
Arguments:
- coverage: int32 [65536, 2048], P(('win', 'trow')), parts along dimension 0, may hold values from 0 to 1, as said below
- dose_level: float32 [65536, 2048], P(('win', 'trow')), parts along dimension 0, may hold values from 0.5 to 2
Outputs:
- dosage: float32 [65536, 2048], P(('win', 'trow')), parts along dimension 0
- exposure: float32 [65536, 2048], P(('win', 'trow')), parts along dimension 0
The draws below stay inside these ranges and needn't reach their ends.
There are 2 independent parts, one for each index of `win`. The reference program is written for one: setup_inputs(seed, part) draws one part's arguments, and reference() takes and returns one part's arrays. A program takes and returns all parts, laid end to end along the dimension named above; each array names one. Nothing has to cross between parts.
Inputs may be any that keep to these rules, and one draw needn't show every extreme that they name: Every aligned 512 x 512 block of pixels holds at least one pixel with coverage 1.
All inputs are finite; a program needn't handle non-finite values.
Results may differ from the reference program's by a relative error of at most 0.00018.
Values sent between devices are 32-bit elements; how exact they have to be, the bound alone decides.
A program may use at most 64 MiB of HBM per device.

```python
import math
import jax
import jax.numpy as jnp
from jax import lax

COLS = 2048
R = 128
BLOCK = 128
F = 512
SIG_FWD = 5
SIG_MID = 50
SIG_BACK = 3000
OUTER = 2
INNER = 2
NROWS = 32768


def expand_blocks(values, size):
    return jnp.repeat(jnp.repeat(values, size, axis=0), size, axis=1)


def draw_coverage(key, part):
    tile = F // 4
    offset_key = jax.random.fold_in(key, 11)
    pixel_key = jax.random.fold_in(key, 12)
    anchor_key = jax.random.fold_in(key, 13)
    parity_key = jax.random.fold_in(key, 14)
    offsets = jax.random.randint(offset_key, (NROWS // tile, COLS // tile), -20, 21)
    row_index = jnp.arange(NROWS, dtype=jnp.int32)[:, None]
    col_index = jnp.arange(COLS, dtype=jnp.int32)[None, :]
    parity = jax.random.randint(parity_key, (NROWS // R + 1,), 0, 2)
    phase = jnp.take(parity, (row_index // R).astype(jnp.int32))
    line_rows = (row_index + phase) % 2 == 0
    dense_half = row_index < NROWS // 2
    base = jnp.where(dense_half, jnp.where(line_rows, 960, 60), 40)
    levels = jnp.clip(base + expand_blocks(offsets, tile), 5, 995)
    draws = jax.random.randint(pixel_key, (NROWS, COLS), 0, 1000)
    covered = draws < levels
    anchors = jax.random.randint(anchor_key, (2, NROWS // F, COLS // F), 0, F)
    anchored = (row_index % F == expand_blocks(anchors[0], F)) & (col_index % F == expand_blocks(anchors[1], F))
    return jnp.where(covered | anchored, 1, 0).astype(jnp.int32)


def draw_dose_level(key, part):
    uniform_part = jax.random.uniform(jax.random.fold_in(key, 21), (NROWS, COLS), jnp.float32)
    result = jnp.exp(jnp.log(0.5) + jnp.log(4.0) * uniform_part)
    return jnp.clip(result, 0.5, 2.0).astype(jnp.float32)


def setup_inputs(seed: int = 0, part: int = 0) -> dict:
    splits = jax.random.split(jax.random.key(seed), 3)
    own_keys = jax.random.split(jax.random.fold_in(splits[2], part), 3)
    return {
        "coverage": draw_coverage(jax.random.fold_in(jax.random.fold_in(splits[2], part), 71), part),
        "dose_level": draw_dose_level(jax.random.fold_in(jax.random.fold_in(splits[2], part), 71), part),
    }


highest = lax.Precision.HIGHEST
backscatter_ratio = 0.7

def raw_profile(offset):
    first = 0.5 * jnp.exp(-offset * offset / (2.0 * SIG_FWD ** 2)) / SIG_FWD
    second = 0.5 * jnp.exp(-offset * offset / (2.0 * SIG_MID ** 2)) / SIG_MID
    return first + second

def short_weight(offset):
    support = jnp.arange(-R, R + 1, dtype=jnp.float32)
    normal = jnp.sum(raw_profile(support))
    return jnp.where(jnp.abs(offset) <= R, raw_profile(offset) / normal, 0.0)

def back_weight(offset):
    spacing = offset * F
    return F * jnp.exp(-spacing * spacing / (2.0 * SIG_BACK ** 2)) / (math.sqrt(2.0 * math.pi) * SIG_BACK)

def smooth_columns(field):
    leading = field.shape[:-1]
    count = field.shape[-1] // BLOCK
    blocked = field.reshape(leading + (count, BLOCK))
    zero_block = jnp.zeros(leading + (1, BLOCK), field.dtype)
    before = jnp.concatenate([zero_block, blocked[..., :-1, :]], axis=-2)
    after = jnp.concatenate([blocked[..., 1:, :], zero_block], axis=-2)
    framed = jnp.concatenate([before[..., BLOCK - R:], blocked, after[..., :R]], axis=-1)
    inner_index = jnp.arange(BLOCK + 2 * R, dtype=jnp.float32)[:, None]
    outer_index = jnp.arange(BLOCK, dtype=jnp.float32)[None, :]
    matrix = short_weight(inner_index - R - outer_index)
    result = jnp.einsum('...bp,pq->...bq', framed, matrix, precision=highest)
    return result.reshape(field.shape)

def short_range(dosage):
    vertical = smooth_columns(dosage.T).T
    return smooth_columns(vertical)

def reference(coverage, dose_level):
    target = jnp.where(coverage == 1, dose_level, 0.0)
    dosage = target
    coarse_count = coverage.shape[0] // F
    coarse_width = coverage.shape[1] // F
    row_ids = jnp.arange(coarse_count, dtype=jnp.float32)
    col_ids = jnp.arange(coarse_width, dtype=jnp.float32)
    vertical_kernel = back_weight(row_ids[:, None] - row_ids[None, :])
    lateral_kernel = back_weight(col_ids[:, None] - col_ids[None, :])
    exposure = dosage
    for outer_step in range(OUTER):
        coarse = dosage.reshape(coarse_count, F, coarse_width, F).sum(axis=(1, 3)) / (F * F)
        lateral = jnp.dot(coarse, lateral_kernel, precision=highest)
        backscatter = jnp.dot(vertical_kernel, lateral, precision=highest)
        spread = jnp.broadcast_to(backscatter[:, None, :, None], (coarse_count, F, coarse_width, F)).reshape(dosage.shape)
        for inner_step in range(INNER):
            exposure = short_range(dosage) + backscatter_ratio * spread
            dosage = dosage * target / exposure
    return (dosage, exposure)
```

```python
import functools
import math

import jax
import jax.numpy as jnp
import numpy as np
from jax import lax
from jax.experimental import pallas as pl
from jax.experimental.pallas import tpu as pltpu
from jax.sharding import PartitionSpec as P

R = 128
F = 512
SIG_FWD = 5
SIG_MID = 50
SIG_BACK = 3000
OUTER = 2
INNER = 2
PASSES = OUTER * INNER
CB = 256
LANES = 128
backscatter_ratio = 0.7
MESH = pl.DeviceIdType.MESH


def raw_profile(offset):
    first = 0.5 * np.exp(-offset * offset / (2.0 * SIG_FWD**2)) / SIG_FWD
    second = 0.5 * np.exp(-offset * offset / (2.0 * SIG_MID**2)) / SIG_MID
    return first + second


def short_weight(offset):
    normal = np.sum(raw_profile(np.arange(-R, R + 1, dtype=np.float64)))
    return np.where(np.abs(offset) <= R, raw_profile(offset) / normal, 0.0)


def back_weight(offset):
    spacing = offset * F
    return (
        F
        * np.exp(-spacing * spacing / (2.0 * SIG_BACK**2))
        / (math.sqrt(2.0 * math.pi) * SIG_BACK)
    )


def two_parts(matrix):
    whole = jnp.asarray(matrix, jnp.float32)
    high = whole.astype(jnp.bfloat16)
    low = (whole - high.astype(jnp.float32)).astype(jnp.bfloat16)
    return high, low


def vertical_matrix(rows):
    out = np.arange(rows, dtype=np.float64)[:, None]
    own = np.arange(rows, dtype=np.float64)
    above = np.arange(-R, 0, dtype=np.float64)
    below = np.arange(rows, rows + R, dtype=np.float64)
    return short_weight(out - np.concatenate([own, above, below])[None, :])


def horizontal_matrix():
    inner = np.arange(CB + 2 * R, dtype=np.float64)[:, None]
    outer = np.arange(CB, dtype=np.float64)[None, :]
    return short_weight(inner - R - outer)


def split(value):
    high = value.astype(jnp.bfloat16)
    low = (value - high.astype(jnp.float32)).astype(jnp.bfloat16)
    return high, low


def dot(left, right):
    return jnp.dot(left, right, preferred_element_type=jnp.float32)


def kernel(
    n, nx, ny,
    cov_hbm, dose_hbm, ah_hbm, al_hbm, bh_hbm, bl_hbm, gtab_hbm,
    dout_hbm, eout_hbm,
    cov, dose, ah, al, bh, bl, gtab,
    dbuf, dh, dl, up, down, vh, vl, dout, eout,
    accs, spread, row_out, row_in, yrows, xout, xrows,
    load_sem, const_sem, out_sem,
    up_send, down_send, up_recv, down_recv,
    a_send, a_recv, y_send, y_recv, x_send, x_recv,
):
    height, width = cov.shape
    blocks = width // CB
    cells = width // F
    group = LANES // cells
    me = lax.axis_index("trow")
    chip, core = me // 2, me % 2
    y, x = chip // nx, chip % nx
    partner = me + 1 - 2 * core
    has_up, has_down = me > 0, me < n - 1
    fwd, bwd = nx // 2, (nx - 1) // 2

    def device(yy, xx, cc):
        return (yy * nx + xx) * 2 + cc

    def load(b):
        cols = pl.ds(b * CB, CB)
        return (
            pltpu.make_async_copy(cov_hbm.at[:, cols], cov.at[:, cols], load_sem.at[0, b]),
            pltpu.make_async_copy(dose_hbm.at[:, cols], dose.at[:, cols], load_sem.at[1, b]),
        )

    for b in range(blocks):
        for copy in load(b):
            copy.start()
    consts = [
        pltpu.make_async_copy(source, target, const_sem.at[k])
        for k, (source, target) in enumerate(
            [(ah_hbm, ah), (al_hbm, al), (bh_hbm, bh), (bl_hbm, bl), (gtab_hbm, gtab)]
        )
    ]
    for copy in consts:
        copy.start()

    barrier = pltpu.get_barrier_semaphore()

    def greet(other):
        pl.semaphore_signal(barrier, inc=1, device_id={"trow": other}, device_id_type=MESH)

    @pl.when(has_up)
    def _():
        greet(me - 1)

    @pl.when(has_down)
    def _():
        greet(me + 1)

    for d in range(1, ny):
        greet(device((y + d) % ny, x, core))
    for d in range(1, fwd + 1):
        greet(device(y, (x + nx - d) % nx, 0))
    for d in range(1, bwd + 1):
        greet(device(y, (x + d) % nx, 1))

    zero_pad = jnp.zeros((height, R), jnp.bfloat16)
    for part in (vh, vl):
        part[:, 0:R] = zero_pad
        part[:, R + width : R + width + R] = zero_pad

    @pl.when(me == 0)
    def _():
        up[...] = jnp.zeros_like(up)

    @pl.when(me == n - 1)
    def _():
        down[...] = jnp.zeros_like(down)

    accs[...] = jnp.zeros_like(accs)
    pl.semaphore_wait(
        barrier,
        has_up.astype(jnp.int32)
        + has_down.astype(jnp.int32)
        + (ny - 1)
        + 2 * jnp.where(core == 0, fwd, bwd),
    )

    def up_copy(p, cols, b):
        return pltpu.make_async_remote_copy(
            src_ref=dbuf.at[p, pl.ds(0, R), cols],
            dst_ref=down.at[p, :, cols],
            send_sem=up_send.at[p],
            recv_sem=down_recv.at[p, b],
            device_id={"trow": me - 1},
            device_id_type=MESH,
        )

    def down_copy(p, cols, b):
        return pltpu.make_async_remote_copy(
            src_ref=dbuf.at[p, pl.ds(height - R, R), cols],
            dst_ref=up.at[p, :, cols],
            send_sem=down_send.at[p],
            recv_sem=up_recv.at[p, b],
            device_id={"trow": me + 1},
            device_id_type=MESH,
        )

    def send_halo(p, b):
        cols = pl.ds(pl.multiple_of(b * CB, CB), CB)

        @pl.when(has_up)
        def _():
            up_copy(p, cols, b).start()

        @pl.when(has_down)
        def _():
            down_copy(p, cols, b).start()

    def wait_halo(p, b):
        cols = pl.ds(pl.multiple_of(b * CB, CB), CB)

        @pl.when(has_up)
        def _():
            down_copy(p, cols, b).wait_recv()

        @pl.when(has_down)
        def _():
            up_copy(p, cols, b).wait_recv()

    def add_cell(b, value):
        part = jnp.sum(value.reshape(height // 8, 8, CB), axis=0)
        accs[b * CB // F] += part[:, :LANES] + part[:, LANES:]

    def keep(p, b, value):
        cols = pl.ds(pl.multiple_of(b * CB, CB), CB)
        dbuf[p, :, cols] = value
        high, low = split(value)
        dh[p % 2, :, cols] = high
        dl[p % 2, :, cols] = low

    def make_target(b, carry):
        cols = pl.ds(pl.multiple_of(b * CB, CB), CB)
        for hbm, buf, k in ((cov_hbm, cov, 0), (dose_hbm, dose, 1)):
            pltpu.make_async_copy(hbm.at[:, cols], buf.at[:, cols], load_sem.at[k, b]).wait()
        target = jnp.where(cov[:, cols] == 1, dose[:, cols], 0.0)
        keep(0, b, target)
        add_cell(b, target)
        send_halo(0, b)
        return carry

    lax.fori_loop(0, blocks, make_target, 0)
    for copy in consts:
        copy.wait()

    lane = lax.broadcasted_iota(jnp.int32, (1, LANES), 1) // group

    def coarse(o):
        row = jnp.zeros((1, LANES), jnp.float32)
        for e in range(cells):
            weight = jnp.zeros((1, LANES), jnp.float32)
            for c in range(cells):
                weight = jnp.where(lane == c, float(back_weight(float(e - c)) / (F * F)), weight)
            row = row + jnp.sum(accs[e], axis=(0, 1), keepdims=True) * weight
        row_out[o] = row
        first = pltpu.make_async_remote_copy(
            src_ref=row_out.at[o],
            dst_ref=row_in.at[o],
            send_sem=a_send.at[o],
            recv_sem=a_recv.at[o],
            device_id={"trow": partner},
            device_id_type=MESH,
        )
        first.start()
        first.wait_recv()
        yrows[o, y] = row + row_in[o]
        for d in range(1, ny):
            pltpu.make_async_remote_copy(
                src_ref=yrows.at[o, y],
                dst_ref=yrows.at[o, y],
                send_sem=y_send.at[o],
                recv_sem=y_recv.at[o],
                device_id={"trow": device((y + d) % ny, x, core)},
                device_id_type=MESH,
            ).start()
        several_y(o).wait_recv()

        def toward(xx):
            total = jnp.zeros((1, LANES), jnp.float32)
            for yy in range(ny):
                total = total + gtab[(y - yy) * nx + xx - x + (nx * ny - 1)] * yrows[o, yy]
            return total

        def send_x(d, k):
            xx = (x + d) % nx
            xout[o, k] = toward(xx)
            for cc in range(2):
                pltpu.make_async_remote_copy(
                    src_ref=xout.at[o, k],
                    dst_ref=xrows.at[o, x],
                    send_sem=x_send.at[o],
                    recv_sem=x_recv.at[o],
                    device_id={"trow": device(y, xx, cc)},
                    device_id_type=MESH,
                ).start()

        @pl.when(core == 0)
        def _():
            for d in range(fwd, 0, -1):
                send_x(d, d - 1)

        @pl.when(core == 1)
        def _():
            for d in range(bwd, 0, -1):
                send_x(nx - d, d - 1)

        xrows[o, x] = toward(x)
        several_x(o, nx - 1).wait_recv()
        total = jnp.zeros((1, LANES), jnp.float32)
        for xx in range(nx):
            total = total + xrows[o, xx]
        total = total * backscatter_ratio
        for c in range(cells):
            spread[c] = jnp.broadcast_to(total[:, c * group : c * group + 1], (8, LANES))

    def several_y(o):
        return pltpu.make_async_remote_copy(
            src_ref=yrows.at[o, pl.ds(0, ny - 1)],
            dst_ref=yrows.at[o, pl.ds(0, ny - 1)],
            send_sem=y_send.at[o],
            recv_sem=y_recv.at[o],
            device_id={"trow": partner},
            device_id_type=MESH,
        )

    def several_x(o, count):
        return pltpu.make_async_remote_copy(
            src_ref=xrows.at[o, pl.ds(0, count)],
            dst_ref=xrows.at[o, pl.ds(0, count)],
            send_sem=x_send.at[o],
            recv_sem=x_recv.at[o],
            device_id={"trow": partner},
            device_id_type=MESH,
        )

    def vertical(p, b):
        cols = pl.ds(pl.multiple_of(b * CB, CB), CB)
        wait_halo(p, b)
        halo = jnp.concatenate([up[p, :, cols], down[p, :, cols]], axis=0)
        halo_high, halo_low = split(halo)
        own_high, own_low = dh[p % 2, :, cols], dl[p % 2, :, cols]
        value = (
            dot(ah[:, :height], own_high)
            + dot(ah[:, height:], halo_high)
            + dot(ah[:, :height], own_low)
            + dot(ah[:, height:], halo_low)
            + dot(al[:, :height], own_high)
            + dot(al[:, height:], halo_high)
        )
        high, low = split(value)
        inside = pl.ds(pl.multiple_of(b * CB + R, R), CB)
        vh[:, inside] = high
        vl[:, inside] = low

    def finish(p, b):
        cols = pl.ds(pl.multiple_of(b * CB, CB), CB)
        framed = pl.ds(pl.multiple_of(b * CB, CB), CB + 2 * R)
        high, low = vh[:, framed], vl[:, framed]
        value = dot(high, bh[...]) + dot(low, bh[...]) + dot(high, bl[...])
        far = spread[b * CB // F][0:1]
        exposure = value + jnp.concatenate([far] * (CB // LANES), axis=1)
        dosage = dbuf[p, :, cols] * dbuf[0, :, cols] / exposure
        if p < PASSES - 1:
            keep(p + 1, b, dosage)
            if (p + 1) % INNER == 0:
                add_cell(b, dosage)
            send_halo(p + 1, b)
        else:
            dout[:, cols] = dosage
            eout[:, cols] = exposure
            pltpu.make_async_copy(dout.at[:, cols], dout_hbm.at[:, cols], out_sem.at[0]).start()
            pltpu.make_async_copy(eout.at[:, cols], eout_hbm.at[:, cols], out_sem.at[1]).start()

    for p in range(PASSES):
        if p % INNER == 0:
            coarse(p // INNER)
            accs[...] = jnp.zeros_like(accs)
        vertical(p, 0)

        def step(b, carry, p=p):
            vertical(p, b)
            finish(p, b - 1)
            return carry

        lax.fori_loop(1, blocks, step, 0)
        finish(p, blocks - 1)

    every = pl.ds(0, width)
    for p in range(PASSES):

        @pl.when(has_up)
        def _(p=p):
            up_copy(p, every, 0).wait_send()

        @pl.when(has_down)
        def _(p=p):
            down_copy(p, every, 0).wait_send()

    for o in range(OUTER):
        pltpu.make_async_remote_copy(
            src_ref=row_out.at[o],
            dst_ref=row_in.at[o],
            send_sem=a_send.at[o],
            recv_sem=a_recv.at[o],
            device_id={"trow": partner},
            device_id_type=MESH,
        ).wait_send()
        several_y(o).wait_send()

        @pl.when(core == 0)
        def _(o=o):
            several_x(o, 2 * fwd).wait_send()

        if bwd:

            @pl.when(core == 1)
            def _(o=o):
                several_x(o, 2 * bwd).wait_send()

    pltpu.make_async_copy(dout, dout_hbm, out_sem.at[0]).wait()
    pltpu.make_async_copy(eout, eout_hbm, out_sem.at[1]).wait()


def solution(mesh):
    n = mesh.shape["trow"]
    chips = n // 2
    nx = max(d for d in range(1, math.isqrt(chips) + 1) if chips % d == 0)
    ny = chips // nx

    def per_device(coverage, dose_level):
        height, width = coverage.shape
        blocks, cells = width // CB, width // F
        assert 2 * height == F and width % F == 0 and height == 2 * R
        ah, al = two_parts(vertical_matrix(height))
        bh, bl = two_parts(horizontal_matrix())
        steps = np.arange(2 * chips, dtype=np.float64) - (chips - 1)
        gtab = jnp.asarray(
            np.broadcast_to(back_weight(steps)[:, None, None], (2 * chips, 1, LANES)), jnp.float32
        )
        f32, bf16 = jnp.float32, jnp.bfloat16
        dma = pltpu.SemaphoreType.DMA
        shape = jax.ShapeDtypeStruct((height, width), f32)
        return pl.pallas_call(
            functools.partial(kernel, n, nx, ny),
            out_shape=(shape, shape),
            in_specs=[pl.BlockSpec(memory_space=pl.ANY)] * 7,
            out_specs=(pl.BlockSpec(memory_space=pl.ANY),) * 2,
            scratch_shapes=[
                pltpu.VMEM((height, width), jnp.int32),
                pltpu.VMEM((height, width), f32),
                pltpu.VMEM(ah.shape, bf16),
                pltpu.VMEM(al.shape, bf16),
                pltpu.VMEM(bh.shape, bf16),
                pltpu.VMEM(bl.shape, bf16),
                pltpu.VMEM(gtab.shape, f32),
                pltpu.VMEM((PASSES, height, width), f32),
                pltpu.VMEM((2, height, width), bf16),
                pltpu.VMEM((2, height, width), bf16),
                pltpu.VMEM((PASSES, R, width), f32),
                pltpu.VMEM((PASSES, R, width), f32),
                pltpu.VMEM((height, width + 2 * R), bf16),
                pltpu.VMEM((height, width + 2 * R), bf16),
                pltpu.VMEM((height, width), f32),
                pltpu.VMEM((height, width), f32),
                pltpu.VMEM((cells, 8, LANES), f32),
                pltpu.VMEM((cells, 8, LANES), f32),
                pltpu.VMEM((OUTER, 1, LANES), f32),
                pltpu.VMEM((OUTER, 1, LANES), f32),
                pltpu.VMEM((OUTER, ny, 1, LANES), f32),
                pltpu.VMEM((OUTER, nx, 1, LANES), f32),
                pltpu.VMEM((OUTER, 2 * nx, 1, LANES), f32),
                dma((2, blocks)),
                dma((5,)),
                dma((2,)),
                dma((PASSES,)),
                dma((PASSES,)),
                dma((PASSES, blocks)),
                dma((PASSES, blocks)),
                dma((OUTER,)),
                dma((OUTER,)),
                dma((OUTER,)),
                dma((OUTER,)),
                dma((OUTER,)),
                dma((OUTER,)),
            ],
            compiler_params=pltpu.CompilerParams(
                collective_id=0, has_side_effects=True, vmem_limit_bytes=60 * 2**20
            ),
            name="dose",
        )(coverage, dose_level, ah, al, bh, bl, gtab)

    spec = P(("win", "trow"), None)
    return jax.shard_map(
        per_device, mesh=mesh, in_specs=(spec, spec), out_specs=(spec, spec), check_vma=False
    )
```

```python
import functools
import math

import jax
import jax.numpy as jnp
import numpy as np
from jax import lax
from jax.experimental import pallas as pl
from jax.experimental.pallas import tpu as pltpu
from jax.sharding import PartitionSpec as P

R = 128
F = 512
SIG_FWD = 5
SIG_MID = 50
SIG_BACK = 3000
OUTER = 2
INNER = 2
PASSES = OUTER * INNER
CB = 256
LANES = 128
backscatter_ratio = 0.7
MESH = pl.DeviceIdType.MESH


def raw_profile(offset):
    first = 0.5 * np.exp(-offset * offset / (2.0 * SIG_FWD**2)) / SIG_FWD
    second = 0.5 * np.exp(-offset * offset / (2.0 * SIG_MID**2)) / SIG_MID
    return first + second


def short_weight(offset):
    normal = np.sum(raw_profile(np.arange(-R, R + 1, dtype=np.float64)))
    return np.where(np.abs(offset) <= R, raw_profile(offset) / normal, 0.0)


def back_weight(offset):
    spacing = offset * F
    return (
        F
        * np.exp(-spacing * spacing / (2.0 * SIG_BACK**2))
        / (math.sqrt(2.0 * math.pi) * SIG_BACK)
    )


def two_parts(matrix):
    whole = jnp.asarray(matrix, jnp.float32)
    high = whole.astype(jnp.bfloat16)
    low = (whole - high.astype(jnp.float32)).astype(jnp.bfloat16)
    return high, low


def vertical_matrix(rows):
    out = np.arange(rows, dtype=np.float64)[:, None]
    own = np.arange(rows, dtype=np.float64)
    above = np.arange(-R, 0, dtype=np.float64)
    below = np.arange(rows, rows + R, dtype=np.float64)
    return short_weight(out - np.concatenate([own, above, below])[None, :])


def horizontal_matrix():
    inner = np.arange(CB + 2 * R, dtype=np.float64)[:, None]
    outer = np.arange(CB, dtype=np.float64)[None, :]
    return short_weight(inner - R - outer)


def split(value):
    high = value.astype(jnp.bfloat16)
    low = (value - high.astype(jnp.float32)).astype(jnp.bfloat16)
    return high, low


def dot(left, right):
    return jnp.dot(left, right, preferred_element_type=jnp.float32)


def kernel(
    n, nx, ny,
    cov_hbm, dose_hbm, ah_hbm, al_hbm, bh_hbm, bl_hbm, gtab_hbm,
    dout, eout,
    cov, dose, ah, al, bh, bl, gtab,
    field, middle, own_sum, up, down, vh, vl,
    accs, spread, row_out, row_in, yrows, xout, xrows,
    load_sem, const_sem,
    up_send, down_send, up_recv, down_recv,
    a_send, a_recv, y_send, y_recv, x_send, x_recv,
):
    height, width = cov.shape
    blocks = width // CB
    cells = width // F
    group = LANES // cells
    me = lax.axis_index("trow")
    chip, core = me // 2, me % 2
    y, x = chip // nx, chip % nx
    partner = me + 1 - 2 * core
    has_up, has_down = me > 0, me < n - 1
    fwd, bwd = nx // 2, (nx - 1) // 2

    def device(yy, xx, cc):
        return (yy * nx + xx) * 2 + cc

    def load(b):
        cols = pl.ds(b * CB, CB)
        return (
            pltpu.make_async_copy(cov_hbm.at[:, cols], cov.at[:, cols], load_sem.at[0, b]),
            pltpu.make_async_copy(dose_hbm.at[:, cols], dose.at[:, cols], load_sem.at[1, b]),
        )

    for b in range(blocks):
        for copy in load(b):
            copy.start()
    consts = [
        pltpu.make_async_copy(source, target, const_sem.at[k])
        for k, (source, target) in enumerate(
            [(ah_hbm, ah), (al_hbm, al), (bh_hbm, bh), (bl_hbm, bl), (gtab_hbm, gtab)]
        )
    ]
    for copy in consts:
        copy.start()

    barrier = pltpu.get_barrier_semaphore()

    def greet(other):
        pl.semaphore_signal(barrier, inc=1, device_id={"trow": other}, device_id_type=MESH)

    @pl.when(has_up)
    def _():
        greet(me - 1)

    @pl.when(has_down)
    def _():
        greet(me + 1)

    for d in range(1, ny):
        greet(device((y + d) % ny, x, core))
    for d in range(1, fwd + 1):
        greet(device(y, (x + nx - d) % nx, 0))
    for d in range(1, bwd + 1):
        greet(device(y, (x + d) % nx, 1))

    accs[...] = jnp.zeros_like(accs)
    def up_copy(p, cols, b):
        return pltpu.make_async_remote_copy(
            src_ref=field.at[p, pl.ds(0, R), cols],
            dst_ref=down.at[p, :, cols],
            send_sem=up_send.at[p],
            recv_sem=down_recv.at[p, b],
            device_id={"trow": me - 1},
            device_id_type=MESH,
        )

    def down_copy(p, cols, b):
        return pltpu.make_async_remote_copy(
            src_ref=field.at[p, pl.ds(height - R, R), cols],
            dst_ref=up.at[p, :, cols],
            send_sem=down_send.at[p],
            recv_sem=up_recv.at[p, b],
            device_id={"trow": me + 1},
            device_id_type=MESH,
        )

    def send_halo(p, b):
        cols = pl.ds(pl.multiple_of(b * CB, CB), CB)

        @pl.when(has_up)
        def _():
            up_copy(p, cols, b).start()

        @pl.when(has_down)
        def _():
            down_copy(p, cols, b).start()

    def wait_halo(p, b):
        cols = pl.ds(pl.multiple_of(b * CB, CB), CB)

        @pl.when(has_up)
        def _():
            down_copy(p, cols, b).wait_recv()

        @pl.when(has_down)
        def _():
            up_copy(p, cols, b).wait_recv()

    def add_cell(b, value):
        part = jnp.sum(value.reshape(value.shape[0] // 8, 8, CB), axis=0)
        accs[b * CB // F] += part[:, :LANES] + part[:, LANES:]

    chunk = 64

    def make_target(b, carry):
        cols = pl.ds(pl.multiple_of(b * CB, CB), CB)
        for hbm, buf, k in ((cov_hbm, cov, 0), (dose_hbm, dose, 1)):
            pltpu.make_async_copy(hbm.at[:, cols], buf.at[:, cols], load_sem.at[k, b]).wait()
        for r in range(0, height, chunk):
            rows = pl.ds(r, chunk)
            target = jnp.where(cov[rows, cols] == 1, dose[rows, cols], 0.0)
            field[0, rows, cols] = target
            add_cell(b, target)
        return carry

    lax.fori_loop(0, blocks, make_target, 0)
    pl.semaphore_wait(
        barrier,
        has_up.astype(jnp.int32)
        + has_down.astype(jnp.int32)
        + (ny - 1)
        + 2 * jnp.where(core == 0, fwd, bwd),
    )

    lane = lax.broadcasted_iota(jnp.int32, (1, LANES), 1) // group

    def coarse_start(o):
        row = jnp.zeros((1, LANES), jnp.float32)
        for e in range(cells):
            weight = jnp.zeros((1, LANES), jnp.float32)
            for c in range(cells):
                weight = jnp.where(lane == c, float(back_weight(float(e - c)) / (F * F)), weight)
            row = row + jnp.sum(accs[e], axis=(0, 1), keepdims=True) * weight
        row_out[o] = row
        pair(o).start()
        accs[...] = jnp.zeros_like(accs)

    def coarse_y(o):
        pair(o).wait_recv()
        yrows[o, y] = row_out[o] + row_in[o]
        for d in range(1, ny):
            pltpu.make_async_remote_copy(
                src_ref=yrows.at[o, y],
                dst_ref=yrows.at[o, y],
                send_sem=y_send.at[o],
                recv_sem=y_recv.at[o],
                device_id={"trow": device((y + d) % ny, x, core)},
                device_id_type=MESH,
            ).start()

    def coarse_x(o):
        several_y(o).wait_recv()

        def toward(xx, shift):
            total = jnp.zeros((1, LANES), jnp.float32)
            for yy in range(ny):
                total = total + gtab[(y - yy) * nx + xx - x + shift + nx * ny] * yrows[o, yy]
            return total

        def send_x(d, k):
            xx = (x + d) % nx
            here = toward(xx, 0)
            for cc in range(2):
                xout[o, k, cc, 0] = here
                xout[o, k, cc, 1] = toward(xx, 2 * cc - 1)
            for cc in range(2):
                pltpu.make_async_remote_copy(
                    src_ref=xout.at[o, k, cc],
                    dst_ref=xrows.at[o, x],
                    send_sem=x_send.at[o],
                    recv_sem=x_recv.at[o],
                    device_id={"trow": device(y, xx, cc)},
                    device_id_type=MESH,
                ).start()

        @pl.when(core == 0)
        def _():
            for d in range(fwd, 0, -1):
                send_x(d, d - 1)

        @pl.when(core == 1)
        def _():
            for d in range(bwd, 0, -1):
                send_x(nx - d, d - 1)

        xrows[o, x, 0] = toward(x, 0)
        xrows[o, x, 1] = toward(x, 2 * core - 1)

    def coarse_end(o):
        several_x(o, nx - 1).wait_recv()
        for k in range(2):
            total = jnp.zeros((1, LANES), jnp.float32)
            for xx in range(nx):
                total = total + xrows[o, xx, k]
            total = total * backscatter_ratio
            for c in range(cells):
                spread[k, c] = jnp.broadcast_to(total[:, c * group : c * group + 1], (8, LANES))

    def pair(o):
        return pltpu.make_async_remote_copy(
            src_ref=row_out.at[o],
            dst_ref=row_in.at[o],
            send_sem=a_send.at[o],
            recv_sem=a_recv.at[o],
            device_id={"trow": partner},
            device_id_type=MESH,
        )

    def several_y(o):
        return pltpu.make_async_remote_copy(
            src_ref=yrows.at[o, pl.ds(0, ny - 1)],
            dst_ref=yrows.at[o, pl.ds(0, ny - 1)],
            send_sem=y_send.at[o],
            recv_sem=y_recv.at[o],
            device_id={"trow": partner},
            device_id_type=MESH,
        )

    def several_x(o, count):
        return pltpu.make_async_remote_copy(
            src_ref=xrows.at[o, pl.ds(0, count)],
            dst_ref=xrows.at[o, pl.ds(0, count)],
            send_sem=x_send.at[o],
            recv_sem=x_recv.at[o],
            device_id={"trow": partner},
            device_id_type=MESH,
        )

    def columns(b):
        return pl.ds(pl.multiple_of(b * CB, CB), CB)

    def far(which, b):
        row = spread[which, b * CB // F]
        return jnp.concatenate([row] * (CB // LANES), axis=1)[0:1]

    def own_product(value):
        high, low = split(value)
        return (
            dot(ah[:, :height], high) + dot(ah[:, :height], low) + dot(al[:, :height], high)
        )

    def halo_product(above, below):
        high, low = split(jnp.concatenate([above, below], axis=0))
        return (
            dot(ah[:, height:], high) + dot(ah[:, height:], low) + dot(al[:, height:], high)
        )

    def store_vertical(b, value):
        high, low = split(value)
        inside = pl.ds(pl.multiple_of(b * CB + R, R), CB)
        vh[:, inside] = high
        vl[:, inside] = low

    def horizontal(b):
        framed = pl.ds(pl.multiple_of(b * CB, CB), CB + 2 * R)
        high, low = vh[:, framed], vl[:, framed]
        return dot(high, bh[...]) + dot(low, bh[...]) + dot(high, bl[...])

    def first_vertical(p, b):
        cols = columns(b)
        wait_halo(p, b)
        store_vertical(b, own_sum[:, cols] + halo_product(up[p, :, cols], down[p, :, cols]))

    def first_finish(p, b):
        field[p + 1, :, columns(b)] = horizontal(b)
        send_halo(p + 1, b)

    def second_vertical(p, b):
        cols = columns(b)
        wait_halo(p, b)
        here = far(0, b)
        for r in range(0, height, chunk):
            rows = pl.ds(r, chunk)
            middle[rows, cols] = (
                field[p - 1, rows, cols] * field[0, rows, cols] / (field[p, rows, cols] + here)
            )
        edge = []
        for halo, which in ((up, 1 - core), (down, core)):
            edge.append(halo[p - 1, :, cols] * halo[0, :, cols] / (halo[p, :, cols] + far(which, b)))
        store_vertical(b, own_product(middle[:, cols]) + halo_product(*edge))

    def second_finish(p, b):
        cols = columns(b)
        eout[:, cols] = horizontal(b)
        here = far(0, b)
        for r in range(0, height, chunk):
            rows = pl.ds(r, chunk)
            exposure = eout[rows, cols] + here
            dosage = middle[rows, cols] * field[0, rows, cols] / exposure
            if p < PASSES - 1:
                field[p + 1, rows, cols] = dosage
                add_cell(b, dosage)
            else:
                dout[rows, cols] = dosage
                eout[rows, cols] = exposure
        if p < PASSES - 1:
            send_halo(p + 1, b)

    def run(p, vertical, finish):
        vertical(p, 0)

        def step(b, carry):
            vertical(p, b)
            finish(p, b - 1)
            return carry

        lax.fori_loop(1, blocks, step, 0)
        finish(p, blocks - 1)

    coarse_start(0)

    def send_target(b, carry):
        send_halo(0, b)
        return carry

    lax.fori_loop(0, blocks, send_target, 0)
    zero_pad = jnp.zeros((height, R), jnp.bfloat16)
    for part in (vh, vl):
        part[:, 0:R] = zero_pad
        part[:, R + width : R + width + R] = zero_pad

    @pl.when(me == 0)
    def _():
        up[...] = jnp.zeros_like(up)

    @pl.when(me == n - 1)
    def _():
        down[...] = jnp.zeros_like(down)

    for copy in consts:
        copy.wait()

    for o in range(OUTER):
        p = INNER * o
        if o:
            coarse_start(o)
        coarse_y(o)

        def own(b, carry, p=p):
            own_sum[:, columns(b)] = own_product(field[p, :, columns(b)])
            return carry

        lax.fori_loop(0, blocks, own, 0)
        coarse_x(o)
        run(p, first_vertical, first_finish)
        coarse_end(o)
        run(p + 1, second_vertical, second_finish)

    every = pl.ds(0, width)
    for p in range(PASSES):

        @pl.when(has_up)
        def _(p=p):
            up_copy(p, every, 0).wait_send()

        @pl.when(has_down)
        def _(p=p):
            down_copy(p, every, 0).wait_send()

    for o in range(OUTER):
        pair(o).wait_send()
        several_y(o).wait_send()

        @pl.when(core == 0)
        def _(o=o):
            several_x(o, 2 * fwd).wait_send()

        if bwd:

            @pl.when(core == 1)
            def _(o=o):
                several_x(o, 2 * bwd).wait_send()


def solution(mesh):
    n = mesh.shape["trow"]
    chips = n // 2
    nx = max(d for d in range(1, math.isqrt(chips) + 1) if chips % d == 0)
    ny = chips // nx

    def per_device(coverage, dose_level):
        height, width = coverage.shape
        blocks, cells = width // CB, width // F
        assert 2 * height == F and width % F == 0 and height == 2 * R
        ah, al = two_parts(vertical_matrix(height))
        bh, bl = two_parts(horizontal_matrix())
        steps = np.arange(2 * chips + 1, dtype=np.float64) - chips
        gtab = jnp.asarray(
            np.broadcast_to(back_weight(steps)[:, None, None], (2 * chips + 1, 1, LANES)), jnp.float32
        )
        f32, bf16 = jnp.float32, jnp.bfloat16
        dma = pltpu.SemaphoreType.DMA
        dosage, exposure = pl.pallas_call(
            functools.partial(kernel, n, nx, ny),
            out_shape=(pltpu.VMEM((height, width), f32), pltpu.VMEM((height, width), f32)),
            in_specs=[pl.BlockSpec(memory_space=pl.ANY)] * 7,
            out_specs=(pl.BlockSpec(memory_space=pltpu.VMEM),) * 2,
            scratch_shapes=[
                pltpu.VMEM((height, width), jnp.int32),
                pltpu.VMEM((height, width), f32),
                pltpu.VMEM(ah.shape, bf16),
                pltpu.VMEM(al.shape, bf16),
                pltpu.VMEM(bh.shape, bf16),
                pltpu.VMEM(bl.shape, bf16),
                pltpu.VMEM(gtab.shape, f32),
                pltpu.VMEM((PASSES, height, width), f32),
                pltpu.VMEM((height, width), f32),
                pltpu.VMEM((height, width), f32),
                pltpu.VMEM((PASSES, R, width), f32),
                pltpu.VMEM((PASSES, R, width), f32),
                pltpu.VMEM((height, width + 2 * R), bf16),
                pltpu.VMEM((height, width + 2 * R), bf16),
                pltpu.VMEM((cells, 8, LANES), f32),
                pltpu.VMEM((2, cells, 8, LANES), f32),
                pltpu.VMEM((OUTER, 1, LANES), f32),
                pltpu.VMEM((OUTER, 1, LANES), f32),
                pltpu.VMEM((OUTER, ny, 1, LANES), f32),
                pltpu.VMEM((OUTER, nx, 2, 2, 1, LANES), f32),
                pltpu.VMEM((OUTER, 2 * nx, 2, 1, LANES), f32),
                dma((2, blocks)),
                dma((5,)),
                dma((PASSES,)),
                dma((PASSES,)),
                dma((PASSES, blocks)),
                dma((PASSES, blocks)),
                dma((OUTER,)),
                dma((OUTER,)),
                dma((OUTER,)),
                dma((OUTER,)),
                dma((OUTER,)),
                dma((OUTER,)),
            ],
            compiler_params=pltpu.CompilerParams(
                collective_id=0, has_side_effects=True, vmem_limit_bytes=(59 * 2 + 1) * 2**19
            ),
            name="dose",
        )(coverage, dose_level, ah, al, bh, bl, gtab)
        return dosage, exposure

    spec = P(("win", "trow"), None)
    return jax.shard_map(
        per_device, mesh=mesh, in_specs=(spec, spec), out_specs=(spec, spec), check_vma=False
    )
```

```python
import functools
import math

import jax
import jax.numpy as jnp
import numpy as np
from jax import lax
from jax.experimental import pallas as pl
from jax.experimental.pallas import tpu as pltpu
from jax.sharding import PartitionSpec as P

R = 128
F = 512
SIG_FWD = 5
SIG_MID = 50
SIG_BACK = 3000
OUTER = 2
INNER = 2
PASSES = OUTER * INNER
CB = 256
LANES = 128
backscatter_ratio = 0.7
MESH = pl.DeviceIdType.MESH


def raw_profile(offset):
    first = 0.5 * np.exp(-offset * offset / (2.0 * SIG_FWD**2)) / SIG_FWD
    second = 0.5 * np.exp(-offset * offset / (2.0 * SIG_MID**2)) / SIG_MID
    return first + second


def short_weight(offset):
    normal = np.sum(raw_profile(np.arange(-R, R + 1, dtype=np.float64)))
    return np.where(np.abs(offset) <= R, raw_profile(offset) / normal, 0.0)


def back_weight(offset):
    spacing = offset * F
    return (
        F
        * np.exp(-spacing * spacing / (2.0 * SIG_BACK**2))
        / (math.sqrt(2.0 * math.pi) * SIG_BACK)
    )


def two_parts(matrix):
    whole = jnp.asarray(matrix, jnp.float32)
    high = whole.astype(jnp.bfloat16)
    low = (whole - high.astype(jnp.float32)).astype(jnp.bfloat16)
    return high, low


def vertical_matrix(rows):
    out = np.arange(rows, dtype=np.float64)[:, None]
    own = np.arange(rows, dtype=np.float64)
    above = np.arange(-R, 0, dtype=np.float64)
    below = np.arange(rows, rows + R, dtype=np.float64)
    return short_weight(out - np.concatenate([own, above, below])[None, :])


def horizontal_matrix():
    inner = np.arange(CB + 2 * R, dtype=np.float64)[:, None]
    outer = np.arange(CB, dtype=np.float64)[None, :]
    return short_weight(inner - R - outer)


def split(value):
    high = value.astype(jnp.bfloat16)
    low = (value - high.astype(jnp.float32)).astype(jnp.bfloat16)
    return high, low


def dot(left, right):
    return jnp.dot(left, right, preferred_element_type=jnp.float32)


def kernel(
    n, nx, ny,
    cov_hbm, dose_hbm, ah_hbm, al_hbm, bh_hbm, bl_hbm, gtab_hbm,
    dout, eout,
    cov, dose, ah, al, bh, bl, gtab,
    field, middle, own_sum, up, down, vh, vl,
    accs, spread, row_out, row_in, yrows, xout, xrows,
    load_sem, const_sem,
    up_send, down_send, up_recv, down_recv,
    a_send, a_recv, y_send, y_recv, x_send, x_recv,
):
    height, width = cov.shape
    blocks = width // CB
    cells = width // F
    group = LANES // cells
    me = lax.axis_index("trow")
    chip, core = me // 2, me % 2
    y, x = chip // nx, chip % nx
    partner = me + 1 - 2 * core
    has_up, has_down = me > 0, me < n - 1
    fwd, bwd = (nx - 1) // 2, nx // 2

    def device(yy, xx, cc):
        return (yy * nx + xx) * 2 + cc

    def load(b):
        cols = pl.ds(b * CB, CB)
        return (
            pltpu.make_async_copy(cov_hbm.at[:, cols], cov.at[:, cols], load_sem.at[0, b]),
            pltpu.make_async_copy(dose_hbm.at[:, cols], dose.at[:, cols], load_sem.at[1, b]),
        )

    for b in range(blocks):
        for copy in load(b):
            copy.start()
    consts = [
        pltpu.make_async_copy(source, target, const_sem.at[k])
        for k, (source, target) in enumerate(
            [(ah_hbm, ah), (al_hbm, al), (bh_hbm, bh), (bl_hbm, bl), (gtab_hbm, gtab)]
        )
    ]
    for copy in consts:
        copy.start()

    barrier = pltpu.get_barrier_semaphore()

    def greet(other):
        pl.semaphore_signal(barrier, inc=1, device_id={"trow": other}, device_id_type=MESH)

    @pl.when(has_up)
    def _():
        greet(me - 1)

    @pl.when(has_down)
    def _():
        greet(me + 1)

    for d in range(1, ny):
        greet(device((y + d) % ny, x, core))
    for d in range(1, fwd + 1):
        greet(device(y, (x + nx - d) % nx, 0))
    for d in range(1, bwd + 1):
        greet(device(y, (x + d) % nx, 1))

    accs[...] = jnp.zeros_like(accs)
    def up_copy(p, cols, b):
        return pltpu.make_async_remote_copy(
            src_ref=field.at[p, pl.ds(0, R), cols],
            dst_ref=down.at[p, :, cols],
            send_sem=up_send.at[p],
            recv_sem=down_recv.at[p, b],
            device_id={"trow": me - 1},
            device_id_type=MESH,
        )

    def down_copy(p, cols, b):
        return pltpu.make_async_remote_copy(
            src_ref=field.at[p, pl.ds(height - R, R), cols],
            dst_ref=up.at[p, :, cols],
            send_sem=down_send.at[p],
            recv_sem=up_recv.at[p, b],
            device_id={"trow": me + 1},
            device_id_type=MESH,
        )

    def send_halo(p, b):
        cols = pl.ds(pl.multiple_of(b * CB, CB), CB)

        @pl.when(has_up)
        def _():
            up_copy(p, cols, b).start()

        @pl.when(has_down)
        def _():
            down_copy(p, cols, b).start()

    def wait_halo(p, b):
        cols = pl.ds(pl.multiple_of(b * CB, CB), CB)

        @pl.when(has_up)
        def _():
            down_copy(p, cols, b).wait_recv()

        @pl.when(has_down)
        def _():
            up_copy(p, cols, b).wait_recv()

    def add_cell(b, value):
        part = jnp.sum(value.reshape(value.shape[0] // 8, 8, CB), axis=0)
        accs[b * CB // F] += part[:, :LANES] + part[:, LANES:]

    chunk = 64

    def make_target(b, carry):
        cols = pl.ds(pl.multiple_of(b * CB, CB), CB)
        for hbm, buf, k in ((cov_hbm, cov, 0), (dose_hbm, dose, 1)):
            pltpu.make_async_copy(hbm.at[:, cols], buf.at[:, cols], load_sem.at[k, b]).wait()
        for r in range(0, height, chunk):
            rows = pl.ds(r, chunk)
            target = jnp.where(cov[rows, cols] == 1, dose[rows, cols], 0.0)
            field[0, rows, cols] = target
            add_cell(b, target)
        return carry

    lax.fori_loop(0, blocks, make_target, 0)
    pl.semaphore_wait(
        barrier,
        has_up.astype(jnp.int32)
        + has_down.astype(jnp.int32)
        + (ny - 1)
        + 2 * jnp.where(core == 0, fwd, bwd),
    )

    lane = lax.broadcasted_iota(jnp.int32, (1, LANES), 1) // group

    def coarse_start(o):
        row = jnp.zeros((1, LANES), jnp.float32)
        for e in range(cells):
            weight = jnp.zeros((1, LANES), jnp.float32)
            for c in range(cells):
                weight = jnp.where(lane == c, float(back_weight(float(e - c)) / (F * F)), weight)
            row = row + jnp.sum(accs[e], axis=(0, 1), keepdims=True) * weight
        row_out[o] = row
        pair(o).start()
        accs[...] = jnp.zeros_like(accs)

    def coarse_y(o):
        pair(o).wait_recv()
        yrows[o, y] = row_out[o] + row_in[o]
        for d in range(1, ny):
            pltpu.make_async_remote_copy(
                src_ref=yrows.at[o, y],
                dst_ref=yrows.at[o, y],
                send_sem=y_send.at[o],
                recv_sem=y_recv.at[o],
                device_id={"trow": device((y + d) % ny, x, core)},
                device_id_type=MESH,
            ).start()

    def coarse_x(o):
        several_y(o).wait_recv()

        def toward(xx, shift):
            total = jnp.zeros((1, LANES), jnp.float32)
            for yy in range(ny):
                total = total + gtab[(y - yy) * nx + xx - x + shift + nx * ny] * yrows[o, yy]
            return total

        def send_x(d, k):
            xx = (x + d) % nx
            here = toward(xx, 0)
            for cc in range(2):
                xout[o, k, cc, 0] = here
                xout[o, k, cc, 1] = toward(xx, 2 * cc - 1)
            for cc in range(2):
                pltpu.make_async_remote_copy(
                    src_ref=xout.at[o, k, cc],
                    dst_ref=xrows.at[o, x],
                    send_sem=x_send.at[o],
                    recv_sem=x_recv.at[o],
                    device_id={"trow": device(y, xx, cc)},
                    device_id_type=MESH,
                ).start()

        @pl.when(core == 0)
        def _():
            for d in range(fwd, 0, -1):
                send_x(d, d - 1)

        @pl.when(core == 1)
        def _():
            for d in range(bwd, 0, -1):
                send_x(nx - d, d - 1)

        xrows[o, x, 0] = toward(x, 0)
        xrows[o, x, 1] = toward(x, 2 * core - 1)

    def coarse_end(o):
        several_x(o, nx - 1).wait_recv()
        for k in range(2):
            total = jnp.zeros((1, LANES), jnp.float32)
            for xx in range(nx):
                total = total + xrows[o, xx, k]
            total = total * backscatter_ratio
            for c in range(cells):
                spread[k, c] = jnp.broadcast_to(total[:, c * group : c * group + 1], (8, LANES))

    def pair(o):
        return pltpu.make_async_remote_copy(
            src_ref=row_out.at[o],
            dst_ref=row_in.at[o],
            send_sem=a_send.at[o],
            recv_sem=a_recv.at[o],
            device_id={"trow": partner},
            device_id_type=MESH,
        )

    def several_y(o):
        return pltpu.make_async_remote_copy(
            src_ref=yrows.at[o, pl.ds(0, ny - 1)],
            dst_ref=yrows.at[o, pl.ds(0, ny - 1)],
            send_sem=y_send.at[o],
            recv_sem=y_recv.at[o],
            device_id={"trow": partner},
            device_id_type=MESH,
        )

    def several_x(o, count):
        return pltpu.make_async_remote_copy(
            src_ref=xrows.at[o, pl.ds(0, count)],
            dst_ref=xrows.at[o, pl.ds(0, count)],
            send_sem=x_send.at[o],
            recv_sem=x_recv.at[o],
            device_id={"trow": partner},
            device_id_type=MESH,
        )

    def columns(b):
        return pl.ds(pl.multiple_of(b * CB, CB), CB)

    def far(which, b):
        row = spread[which, b * CB // F]
        return jnp.concatenate([row] * (CB // LANES), axis=1)[0:1]

    def own_product(value):
        high, low = split(value)
        return (
            dot(ah[:, :height], high) + dot(ah[:, :height], low) + dot(al[:, :height], high)
        )

    def halo_product(above, below):
        high, low = split(jnp.concatenate([above, below], axis=0))
        return (
            dot(ah[:, height:], high) + dot(ah[:, height:], low) + dot(al[:, height:], high)
        )

    def store_vertical(b, value):
        high, low = split(value)
        inside = pl.ds(pl.multiple_of(b * CB + R, R), CB)
        vh[:, inside] = high
        vl[:, inside] = low

    def horizontal(b):
        framed = pl.ds(pl.multiple_of(b * CB, CB), CB + 2 * R)
        high, low = vh[:, framed], vl[:, framed]
        return dot(high, bh[...]) + dot(low, bh[...]) + dot(high, bl[...])

    def first_vertical(p, b):
        cols = columns(b)
        wait_halo(p, b)
        store_vertical(b, own_sum[:, cols] + halo_product(up[p, :, cols], down[p, :, cols]))

    def first_finish(p, b):
        field[p + 1, :, columns(b)] = horizontal(b)
        send_halo(p + 1, b)

    def second_vertical(p, b):
        cols = columns(b)
        wait_halo(p, b)
        here = far(0, b)
        for r in range(0, height, chunk):
            rows = pl.ds(r, chunk)
            middle[rows, cols] = (
                field[p - 1, rows, cols] * field[0, rows, cols] / (field[p, rows, cols] + here)
            )
        edge = []
        for halo, which in ((up, 1 - core), (down, core)):
            edge.append(halo[p - 1, :, cols] * halo[0, :, cols] / (halo[p, :, cols] + far(which, b)))
        store_vertical(b, own_product(middle[:, cols]) + halo_product(*edge))

    def second_finish(p, b):
        cols = columns(b)
        eout[:, cols] = horizontal(b)
        here = far(0, b)
        for r in range(0, height, chunk):
            rows = pl.ds(r, chunk)
            exposure = eout[rows, cols] + here
            dosage = middle[rows, cols] * field[0, rows, cols] / exposure
            if p < PASSES - 1:
                field[p + 1, rows, cols] = dosage
                add_cell(b, dosage)
            else:
                dout[rows, cols] = dosage
                eout[rows, cols] = exposure
        if p < PASSES - 1:
            send_halo(p + 1, b)

    def run(p, vertical, finish, first, last):
        if first == 0:
            vertical(p, 0)
            first = 1

        def step(b, carry):
            vertical(p, b)
            finish(p, b - 1)
            return carry

        lax.fori_loop(first, last, step, 0)
        if last == blocks:
            finish(p, blocks - 1)

    coarse_start(0)

    def send_target(b, carry):
        send_halo(0, b)
        return carry

    lax.fori_loop(0, blocks, send_target, 0)
    zero_pad = jnp.zeros((height, R), jnp.bfloat16)
    for part in (vh, vl):
        part[:, 0:R] = zero_pad
        part[:, R + width : R + width + R] = zero_pad

    @pl.when(me == 0)
    def _():
        up[...] = jnp.zeros_like(up)

    @pl.when(me == n - 1)
    def _():
        down[...] = jnp.zeros_like(down)

    for copy in consts:
        copy.wait()

    for o in range(OUTER):
        p = INNER * o
        if o:
            coarse_start(o)
        coarse_y(o)

        def own(b, carry, p=p):
            own_sum[:, columns(b)] = own_product(field[p, :, columns(b)])
            return carry

        lax.fori_loop(0, blocks, own, 0)
        early = 0
        if early:
            run(p, first_vertical, first_finish, 0, early)
        coarse_x(o)
        run(p, first_vertical, first_finish, early, blocks)
        coarse_end(o)
        run(p + 1, second_vertical, second_finish, 0, blocks)

    every = pl.ds(0, width)
    for p in range(PASSES):

        @pl.when(has_up)
        def _(p=p):
            up_copy(p, every, 0).wait_send()

        @pl.when(has_down)
        def _(p=p):
            down_copy(p, every, 0).wait_send()

    for o in range(OUTER):
        pair(o).wait_send()
        several_y(o).wait_send()

        @pl.when(core == 0)
        def _(o=o):
            several_x(o, 2 * fwd).wait_send()

        if bwd:

            @pl.when(core == 1)
            def _(o=o):
                several_x(o, 2 * bwd).wait_send()


def write_out(dout, eout, dout_hbm, eout_hbm, sems):
    copies = [
        pltpu.make_async_copy(dout, dout_hbm, sems.at[0]),
        pltpu.make_async_copy(eout, eout_hbm, sems.at[1]),
    ]
    for copy in copies:
        copy.start()
    for copy in copies:
        copy.wait()


def solution(mesh):
    n = mesh.shape["trow"]
    chips = n // 2
    nx = max(d for d in range(1, math.isqrt(chips) + 1) if chips % d == 0)
    ny = chips // nx

    def per_device(coverage, dose_level):
        height, width = coverage.shape
        blocks, cells = width // CB, width // F
        assert 2 * height == F and width % F == 0 and height == 2 * R
        ah, al = two_parts(vertical_matrix(height))
        bh, bl = two_parts(horizontal_matrix())
        steps = np.arange(2 * chips + 1, dtype=np.float64) - chips
        gtab = jnp.asarray(
            np.broadcast_to(back_weight(steps)[:, None, None], (2 * chips + 1, 1, LANES)), jnp.float32
        )
        f32, bf16 = jnp.float32, jnp.bfloat16
        dma = pltpu.SemaphoreType.DMA
        dosage, exposure = pl.pallas_call(
            functools.partial(kernel, n, nx, ny),
            out_shape=(pltpu.VMEM((height, width), f32), pltpu.VMEM((height, width), f32)),
            in_specs=[pl.BlockSpec(memory_space=pl.ANY)] * 7,
            out_specs=(pl.BlockSpec(memory_space=pltpu.VMEM),) * 2,
            scratch_shapes=[
                pltpu.VMEM((height, width), jnp.int32),
                pltpu.VMEM((height, width), f32),
                pltpu.VMEM(ah.shape, bf16),
                pltpu.VMEM(al.shape, bf16),
                pltpu.VMEM(bh.shape, bf16),
                pltpu.VMEM(bl.shape, bf16),
                pltpu.VMEM(gtab.shape, f32),
                pltpu.VMEM((PASSES, height, width), f32),
                pltpu.VMEM((height, width), f32),
                pltpu.VMEM((height, width), f32),
                pltpu.VMEM((PASSES, R, width), f32),
                pltpu.VMEM((PASSES, R, width), f32),
                pltpu.VMEM((height, width + 2 * R), bf16),
                pltpu.VMEM((height, width + 2 * R), bf16),
                pltpu.VMEM((cells, 8, LANES), f32),
                pltpu.VMEM((2, cells, 8, LANES), f32),
                pltpu.VMEM((OUTER, 1, LANES), f32),
                pltpu.VMEM((OUTER, 1, LANES), f32),
                pltpu.VMEM((OUTER, ny, 1, LANES), f32),
                pltpu.VMEM((OUTER, nx, 2, 2, 1, LANES), f32),
                pltpu.VMEM((OUTER, 2 * nx, 2, 1, LANES), f32),
                dma((2, blocks)),
                dma((5,)),
                dma((PASSES,)),
                dma((PASSES,)),
                dma((PASSES, blocks)),
                dma((PASSES, blocks)),
                dma((OUTER,)),
                dma((OUTER,)),
                dma((OUTER,)),
                dma((OUTER,)),
                dma((OUTER,)),
                dma((OUTER,)),
            ],
            compiler_params=pltpu.CompilerParams(
                collective_id=0, has_side_effects=True, vmem_limit_bytes=(59 * 2 + 1) * 2**19
            ),
            name="dose",
        )(coverage, dose_level, ah, al, bh, bl, gtab)
        shape = jax.ShapeDtypeStruct((height, width), f32)
        return pl.pallas_call(
            write_out,
            out_shape=(shape, shape),
            in_specs=[pl.BlockSpec(memory_space=pl.ANY)] * 2,
            out_specs=(pl.BlockSpec(memory_space=pl.ANY),) * 2,
            scratch_shapes=[dma((2,))],
            compiler_params=pltpu.CompilerParams(vmem_limit_bytes=2**20),
            name="write_out",
        )(dosage, exposure)

    spec = P(("win", "trow"), None)
    return jax.shard_map(
        per_device, mesh=mesh, in_specs=(spec, spec), out_specs=(spec, spec), check_vma=False
    )
```
